128 devices in a mesh: dp: 8 (over x, core), tensor: 16 (over z, y).
Axes of the slice: x: 4, y: 4, z: 4, core: 2. Of those that a mesh axis runs over, the one named last changes fastest.
Arguments:
- tokens: bfloat16 [192, 8, 4096], P('dp'), may hold values from -6 to 6
- norm_gain: float32 [4096], replicated, may hold values from 0.1 to 1.9
- in_weight: bfloat16 [4096, 2, 8192], P(None, None, 'tensor'), may hold values from -0.09375 to 0.09375
- group_weight: bfloat16 [4096, 2048], P(None, 'tensor'), may hold values from -0.09375 to 0.09375
- step_weight: bfloat16 [4096, 128], P(None, 'tensor'), may hold values from -0.09375 to 0.09375
- value_kernel: bfloat16 [4, 8192], P(None, 'tensor'), may hold values from -3 to 3
- value_offset: bfloat16 [8192], P('tensor'), may hold values from -3 to 3
- group_kernel: bfloat16 [4, 2048], P(None, 'tensor'), may hold values from -3 to 3
- group_offset: bfloat16 [2048], P('tensor'), may hold values from -3 to 3
- step_bias: float32 [128], P('tensor'), may hold values from -4 to 1
- decay_rate: float32 [128], P('tensor'), may hold values from 0.05 to 2
- skip_gain: float32 [128], P('tensor'), may hold values from 0.5 to 2
- out_gain: float32 [8192], P('tensor'), may hold values from 0.1 to 1.9
- out_weight: bfloat16 [8192, 4096], P('tensor'), may hold values from -0.0625 to 0.0625
- scan_state: bfloat16 [192, 128, 64, 128], P('dp', 'tensor'), may hold values from -6 to 6
- value_cache: bfloat16 [192, 3, 8192], P('dp', None, 'tensor'), may hold values from -6 to 6
- group_cache: bfloat16 [192, 3, 2048], P('dp', None, 'tensor'), may hold values from -6 to 6
- accepted: int32 [192], P('dp'), may hold values from 0 to 8, as said below
- draft_lengths: int32 [192], P('dp'), may hold values from 1 to 8, as said below
- live_flags: int32 [192], P('dp'), may hold values 0 or 1
Outputs:
- layer_out: bfloat16 [192, 8, 4096], P('dp')
- kept_state: bfloat16 [192, 128, 64, 128], P('dp', 'tensor')
- value_kept: bfloat16 [192, 3, 8192], P('dp', None, 'tensor')
- group_kept: bfloat16 [192, 3, 2048], P('dp', None, 'tensor')
- accepted_total: int32 [1], replicated
The draws below stay inside these ranges and needn't reach their ends.
Inputs may be any that keep to these rules, and one draw needn't show every extreme that they name: `draft_lengths`: positions at or after a request's draft length are padding. `accepted`: never more than the same request's draft length.
All inputs are finite; a program needn't handle non-finite values.
Results may differ from the reference program's by a relative error of at most 0.012.
Values may be sent and summed in bfloat16 or wider, within the bound.
No kernel may reach another device: no remote copies, remote signals or barrier semaphores. Data moves between devices by JAX's collectives and lax.ppermute only.
A program may use at most 128 MiB of HBM per device.

```python
import math
import jax
import jax.numpy as jnp
from jax import lax

D = 4096
STATE = 128
HEADDIM = 64
CONV = 4
DRAFT = 8
REQ_DEV = 24
HEADS = 128
NGROUPS = 8
INNER = 8192
GCOLS = 2048
REQUESTS = 192


def draft_pair(key):
    block_count = REQUESTS // REQ_DEV
    full_row = jax.random.randint(jax.random.fold_in(key, 10), (), 0, REQUESTS)
    short_row = (full_row + 1) % REQUESTS
    block_caps = jax.random.randint(jax.random.fold_in(key, 11), (block_count,), 1, DRAFT + 1)
    block_caps = jnp.where(jnp.arange(block_count) == full_row // REQ_DEV, DRAFT, block_caps)
    per_request = jnp.repeat(block_caps, REQ_DEV, total_repeat_length=REQUESTS)
    lengths = jax.random.randint(jax.random.fold_in(key, 12), (REQUESTS,), 1, per_request + 1)
    row_ids = jnp.arange(REQUESTS)
    lengths = jnp.where(row_ids == full_row, DRAFT, lengths)
    lengths = jnp.where(row_ids == short_row, 1, lengths)
    accepted_counts = jax.random.randint(jax.random.fold_in(key, 13), (REQUESTS,), 0, lengths + 1)
    accepted_counts = jnp.where(row_ids == full_row, DRAFT, accepted_counts)
    accepted_counts = jnp.where(row_ids == short_row, 0, accepted_counts)
    return (lengths.astype(jnp.int32), accepted_counts.astype(jnp.int32))


def draw_draft_lengths(key, part):
    return draft_pair(key)[0]


def draw_accepted(key, part):
    return draft_pair(key)[1]


def plant(array, own_key, smallest, largest):
    extent = array.shape
    index_at = [jax.random.randint(jax.random.fold_in(own_key, axis), (), 0, extent[axis]) for axis in range(len(extent))]
    array = array.at[tuple(index_at)].set(smallest)
    longest = extent.index(max(extent))
    index_at[longest] = (index_at[longest] + 1) % extent[longest]
    return array.at[tuple(index_at)].set(largest)


def block_levels(own_key, dims, cuts, smallest, top_value):
    factor_of, own = 1.0, jax.random.fold_in(own_key, 6)
    for dim, blocks in cuts:
        draws = jnp.exp(jax.random.uniform(jax.random.fold_in(own, dim), (blocks,), jnp.float32, smallest / len(cuts), top_value / len(cuts)))
        factor_of = factor_of * jnp.repeat(draws, dims[dim] // blocks).reshape([-1 if axis == dim else 1 for axis in range(len(dims))])
    return factor_of


def noise(own_key, dims, deviation, most, cuts=(), kind=jnp.bfloat16):
    factor_of = block_levels(own_key, dims, cuts, -0.22, 0.18) if cuts else 1.0
    result = jax.random.normal(own_key, dims, jnp.float32) * deviation * factor_of
    return jnp.minimum(jnp.maximum(result, -most), most).astype(kind)


def setup_inputs(seed: int = 0) -> dict:
    arg_keys = jax.random.split(jax.random.key(seed), 21)
    tokens = noise(arg_keys[0], (REQUESTS, DRAFT, D), 1.0, 6.0, ((0, 8),))
    norm_gain = jnp.clip(1.0 + 0.18 * jax.random.normal(arg_keys[1], (D,), jnp.float32), 0.1, 1.9)
    in_weight = noise(arg_keys[2], (D, 2, INNER), D ** -0.5, 0.09375, ((2, 16),))
    group_weight = noise(arg_keys[3], (D, GCOLS), D ** -0.5, 0.09375, ((1, 16),))
    step_weight = noise(arg_keys[4], (D, HEADS), D ** -0.5, 0.09375, ((1, 16),))
    value_kernel = noise(arg_keys[5], (CONV, INNER), CONV ** -0.5, 3.0, ((1, 16),))
    value_offset = noise(arg_keys[6], (INNER,), 0.5, 3.0, ((0, 16),))
    group_kernel = noise(arg_keys[7], (CONV, GCOLS), CONV ** -0.5, 3.0, ((1, 16),))
    group_offset = noise(arg_keys[8], (GCOLS,), 0.5, 3.0, ((0, 16),))
    step_bias = jnp.clip(-4.0 + 5.0 * jax.random.uniform(arg_keys[9], (HEADS,), jnp.float32) ** block_levels(arg_keys[9], (HEADS,), ((0, 16),), -0.2, 0.2), -4.0, 1.0)
    decay_rate = jnp.clip(jnp.exp(math.log(2.0) - 3.6888794 * jax.random.uniform(arg_keys[10], (HEADS,), jnp.float32) ** block_levels(arg_keys[10], (HEADS,), ((0, 16),), -0.2, 0.2)), 0.05, 2.0)
    skip_gain = jnp.clip(0.5 + 1.5 * jax.random.uniform(arg_keys[11], (HEADS,), jnp.float32) ** block_levels(arg_keys[11], (HEADS,), ((0, 16),), -0.2, 0.2), 0.5, 2.0)
    out_gain = jnp.clip(1.0 + 0.18 * jax.random.normal(arg_keys[12], (INNER,), jnp.float32), 0.1, 1.9)
    out_weight = noise(arg_keys[13], (INNER, D), INNER ** -0.5, 0.0625, ((0, 16),))
    scan_state = noise(arg_keys[14], (REQUESTS, HEADS, HEADDIM, STATE), 1.0, 6.0, ((0, 8), (1, 16)))
    value_cache = noise(arg_keys[15], (REQUESTS, CONV - 1, INNER), 1.0, 6.0, ((0, 8), (2, 16)))
    group_cache = noise(arg_keys[16], (REQUESTS, CONV - 1, GCOLS), 1.0, 6.0, ((0, 8), (2, 16)))
    accepted = draw_accepted(jax.random.fold_in(arg_keys[20], 71), 0)
    draft_lengths = draw_draft_lengths(jax.random.fold_in(arg_keys[20], 71), 0)
    live_flags = plant((jax.random.randint(arg_keys[19], (REQUESTS,), 0, 8) < 7).astype(jnp.int32), jax.random.fold_in(arg_keys[19], 1), 0, 1)
    return {"tokens": tokens, "norm_gain": norm_gain, "in_weight": in_weight, "group_weight": group_weight, "step_weight": step_weight, "value_kernel": value_kernel, "value_offset": value_offset, "group_kernel": group_kernel, "group_offset": group_offset, "step_bias": step_bias, "decay_rate": decay_rate, "skip_gain": skip_gain, "out_gain": out_gain, "out_weight": out_weight, "scan_state": scan_state, "value_cache": value_cache, "group_cache": group_cache, "accepted": accepted, "draft_lengths": draft_lengths, "live_flags": live_flags}


EPSILON = 1e-05

def convolve(window, fresh_rows, kernel, offset):
    sequence = jnp.concatenate([window, fresh_rows], axis=1)
    length = fresh_rows.shape[1]
    summed = jnp.zeros(fresh_rows.shape, jnp.float32) + offset.astype(jnp.float32)
    for tap_index in range(kernel.shape[0]):
        summed = summed + kernel[tap_index].astype(jnp.float32) * sequence[:, tap_index:tap_index + length].astype(jnp.float32)
    return (jax.nn.silu(summed), sequence)

def keep_window(sequence, kept_count, width_rows):
    return jax.vmap(lambda single, start_row: lax.dynamic_slice_in_dim(single, start_row, width_rows, 0))(sequence, kept_count)

def reference(tokens, norm_gain, in_weight, group_weight, step_weight, value_kernel, value_offset, group_kernel, group_offset, step_bias, decay_rate, skip_gain, out_gain, out_weight, scan_state, value_cache, group_cache, accepted, draft_lengths, live_flags):
    flat_rows = tokens.reshape(REQUESTS * DRAFT, D).astype(jnp.float32)
    normed = (flat_rows * lax.rsqrt(lax.optimization_barrier(jnp.mean(flat_rows * flat_rows, axis=1, keepdims=True)) + EPSILON) * norm_gain).astype(jnp.bfloat16)
    inner_proj = jnp.dot(normed, in_weight.reshape(D, 2 * INNER), preferred_element_type=jnp.float32).astype(jnp.bfloat16).reshape(REQUESTS, DRAFT, 2, INNER)
    gate_part = inner_proj[:, :, 0]
    value_part = inner_proj[:, :, 1]
    group_proj = jnp.dot(normed, group_weight, preferred_element_type=jnp.float32).astype(jnp.bfloat16).reshape(REQUESTS, DRAFT, GCOLS)
    step_raw = jnp.dot(normed, step_weight, preferred_element_type=jnp.float32).reshape(REQUESTS, DRAFT, HEADS)
    value_conv, value_seq = convolve(value_cache, value_part, value_kernel, value_offset)
    group_conv, group_seq = convolve(group_cache, group_proj, group_kernel, group_offset)
    group_maps = group_conv.reshape(REQUESTS, DRAFT, NGROUPS, 2, STATE)
    input_maps = group_maps[:, :, :, 0]
    output_maps = group_maps[:, :, :, 1]
    step_size = jax.nn.softplus(step_raw + step_bias)
    decay_step = jnp.exp(-step_size * decay_rate)
    kept_count = accepted * live_flags
    per_group = HEADS // NGROUPS

    def head_scan(head_index):
        values = lax.dynamic_slice_in_dim(value_conv, head_index * HEADDIM, HEADDIM, 2)
        group_index = head_index // per_group
        input_map = lax.dynamic_index_in_dim(input_maps, group_index, 2, keepdims=False)
        output_map = lax.dynamic_index_in_dim(output_maps, group_index, 2, keepdims=False)
        head_decay = lax.dynamic_index_in_dim(decay_step, head_index, 2, keepdims=False)
        head_step = lax.dynamic_index_in_dim(step_size, head_index, 2, keepdims=False)
        initial = lax.dynamic_index_in_dim(scan_state, head_index, 1, keepdims=False).astype(jnp.float32)
        head_skip = lax.dynamic_index_in_dim(skip_gain, head_index, 0, keepdims=False)

        def advance(carry_pair, position):
            current, kept_now = carry_pair
            scaled = (head_step[:, position][:, None] * values[:, position])[:, :, None]
            current = head_decay[:, position][:, None, None] * current + scaled * input_map[:, position][:, None, :]
            produced = lax.optimization_barrier(jnp.sum(current * output_map[:, position][:, None, :], axis=2)) + head_skip * values[:, position]
            kept_now = jnp.where((position < kept_count)[:, None, None], current, kept_now)
            return ((current, kept_now), produced)
        (final_state, kept_now), produced = lax.scan(advance, (initial, initial), jnp.arange(DRAFT, dtype=jnp.int32))
        return (produced, kept_now.astype(jnp.bfloat16))
    produced, kept_heads = lax.map(head_scan, jnp.arange(HEADS, dtype=jnp.int32))
    head_out = jnp.transpose(produced, (2, 1, 0, 3)).reshape(REQUESTS, DRAFT, INNER)
    kept_state = jnp.transpose(kept_heads, (1, 0, 2, 3))
    gated = head_out * jax.nn.silu(gate_part.astype(jnp.float32))
    grouped = gated.reshape(REQUESTS, DRAFT, NGROUPS, INNER // NGROUPS)
    scale_rows = lax.rsqrt(lax.optimization_barrier(jnp.mean(grouped * grouped, axis=3, keepdims=True)) + EPSILON)
    valid_rows = (jnp.arange(DRAFT)[None, :] < draft_lengths[:, None]) & (live_flags[:, None] == 1)
    normalized = jnp.where(valid_rows[:, :, None], (grouped * scale_rows).reshape(REQUESTS, DRAFT, INNER) * out_gain, 0.0).astype(jnp.bfloat16)
    layer_out = jnp.dot(normalized.reshape(REQUESTS * DRAFT, INNER), out_weight, preferred_element_type=jnp.float32).astype(jnp.bfloat16).reshape(REQUESTS, DRAFT, D)
    value_kept = keep_window(value_seq, kept_count, CONV - 1)
    group_kept = keep_window(group_seq, kept_count, CONV - 1)
    accepted_total = jnp.sum(kept_count).astype(jnp.int32).reshape(1)
    return (layer_out, kept_state, value_kept, group_kept, accepted_total)
```

```python
import math

import jax
import jax.numpy as jnp
from jax import lax
from jax.experimental import pallas as pl
from jax.experimental.pallas import tpu as pltpu
from jax.sharding import Mesh
from jax.sharding import PartitionSpec as P

DP = ("dp_0", "dp_1")


EPSILON = 1e-05


ALL = ("dp_0", "dp_1", "tensor")
NEAR = (0, 1, 4, 5)
FAR = (0, 3, 12, 15)
COLS = 256


def swapped(value, axis, mask):
    pairs = [(source, source ^ mask) for source in range(math.prod(lax.axis_size(a) for a in axis))]
    return lax.ppermute(value, axis, pairs)


def exchanged(value, masks):
    tensor = lax.axis_size("tensor")
    total = tensor * lax.axis_size("dp_0") * lax.axis_size("dp_1")
    pairs = [(s, s ^ masks[(s // tensor) % 2]) for s in range(total)]
    return lax.ppermute(value, ALL, pairs)


def chunk_at(outer, inner):
    me = lax.axis_index("tensor")
    core = lax.axis_index("dp_1")
    near = (me ^ (me >> 1)) & 5
    even = near ^ (NEAR[outer] ^ FAR[inner])
    odd = me ^ near ^ (FAR[outer] ^ NEAR[inner])
    return jnp.where(core == 0, even, odd)


def chunk_table():
    return jnp.stack([chunk_at(outer, inner) for outer in range(4) for inner in range(4)])


def out_project(table, gated, scale, out_weight):
    rows, inner_dev = gated.shape

    def body(table_ref, gated_ref, scale_ref, weight_ref, *rest):
        parts, (buffer, sems) = rest[:4], rest[4:]
        copies = []
        for place in range(16):
            start = pl.multiple_of(table_ref[place] * COLS, COLS)
            copies.append(
                pltpu.make_async_copy(
                    weight_ref.at[:, pl.ds(start, COLS)], buffer.at[place], sems.at[place]
                )
            )
        for copy in copies:
            copy.start()
        for place in range(16):
            copies[place].wait()
            part = jnp.dot(gated_ref[...], buffer[place], preferred_element_type=jnp.float32)
            parts[place // 4][place % 4] = (part * scale_ref[...]).astype(jnp.bfloat16)

    whole = pl.BlockSpec(memory_space=pltpu.VMEM)
    return pl.pallas_call(
        body,
        out_shape=[jax.ShapeDtypeStruct((4, rows, COLS), jnp.bfloat16)] * 4,
        in_specs=[
            pl.BlockSpec(memory_space=pltpu.SMEM),
            whole,
            whole,
            pl.BlockSpec(memory_space=pl.ANY),
        ],
        out_specs=[whole] * 4,
        scratch_shapes=[
            pltpu.VMEM((16, inner_dev, COLS), jnp.bfloat16),
            pltpu.SemaphoreType.DMA((16,)),
        ],
        name="out_project",
    )(table, gated, scale, out_weight)


def silu(value):
    return value / (1.0 + jnp.exp(-value))


def shifted_conv(fresh, cache_ref, kernel_ref, offset_ref):
    position = lax.broadcasted_iota(jnp.int32, fresh.shape, 1)
    kernel = kernel_ref[...].astype(jnp.float32)
    cache = [cache_ref[i].astype(jnp.float32)[:, None, :] for i in range(3)]
    summed = fresh * kernel[3:4][None] + offset_ref[...].astype(jnp.float32)[None]
    for back in (1, 2, 3):
        moved = pltpu.roll(fresh, back, axis=1)
        for place in range(back):
            moved = jnp.where(position == place, cache[3 - back + place], moved)
        summed = summed + moved * kernel[3 - back : 4 - back][None]
    return silu(summed)


def enter(tokens, norm_gain, group_weight, step_weight, group_cache, group_kernel, group_offset):
    rows, width = tokens.shape
    cols = group_weight.shape[1]
    heads = step_weight.shape[0]

    def body(
        tok_ref, gain_ref, gw_ref, sw_ref, cache_ref, ker_ref, off_ref,
        normed_ref, proj_ref, conv_ref, step_ref,
    ):
        wide = tok_ref[...].astype(jnp.float32)
        scale = lax.rsqrt(jnp.mean(wide * wide, axis=1, keepdims=True) + EPSILON)
        normed = (wide * scale * gain_ref[...]).astype(jnp.bfloat16)
        normed_ref[...] = normed
        proj = jnp.dot(normed, gw_ref[...], preferred_element_type=jnp.float32)
        proj = proj.astype(jnp.bfloat16)
        proj_ref[...] = proj
        step_ref[...] = lax.dot_general(
            normed, sw_ref[...], (((1,), (1,)), ((), ())), preferred_element_type=jnp.float32
        )
        fresh = proj.astype(jnp.float32).reshape(rows // 8, 8, cols)
        conv_ref[...] = shifted_conv(fresh, cache_ref, ker_ref, off_ref).astype(jnp.bfloat16)

    whole = pl.BlockSpec(memory_space=pltpu.VMEM)
    return pl.pallas_call(
        body,
        out_shape=[
            jax.ShapeDtypeStruct((rows, width), jnp.bfloat16),
            jax.ShapeDtypeStruct((rows, cols), jnp.bfloat16),
            jax.ShapeDtypeStruct((rows // 8, 8, cols), jnp.bfloat16),
            jax.ShapeDtypeStruct((rows, heads), jnp.float32),
        ],
        in_specs=[whole] * 7,
        out_specs=[whole] * 4,
        name="enter",
    )(tokens, norm_gain, group_weight, step_weight, group_cache, group_kernel, group_offset)


def in_project(normed, in_weight):
    rows, width = normed.shape
    half = width // 2
    lane_blocks = in_weight.shape[2] // 128
    inner_dev = in_weight.shape[2]
    chunks = 8
    depth = half // chunks
    viewed = in_weight.reshape(half, 2, 2, lane_blocks, 128).transpose(0, 1, 3, 2, 4)

    def body(normed_ref, weight_ref, gate_ref, value_ref, buffer, sums, sems):
        def copy_of(chunk, parity, block):
            span = pl.ds(chunk * depth, depth)
            return pltpu.make_async_copy(
                weight_ref.at[span, parity, block],
                buffer.at[parity, block, span],
                sems.at[chunk, parity, block],
            )

        places = [(parity, block) for parity in range(2) for block in range(lane_blocks)]
        for chunk in range(chunks):
            for parity, block in places:
                copy_of(chunk, parity, block).start()
        flat = buffer.reshape(2 * lane_blocks * width, 128)
        even = lax.broadcasted_iota(jnp.int32, (rows, 128), 1) % 2 == 0
        for chunk in range(chunks):
            sides = [[], []], [[], []]
            for lane in range(2 * depth * chunk, 2 * depth * (chunk + 1), 128):
                piece = normed_ref[:, lane : lane + 128].astype(jnp.float32)
                first = jnp.where(even, piece, 0.0)
                second = jnp.where(even, 0.0, piece)
                sides[0][0].append(first.astype(jnp.bfloat16))
                sides[0][1].append(pltpu.roll(first, 1, axis=1).astype(jnp.bfloat16))
                sides[1][0].append(pltpu.roll(second, 127, axis=1).astype(jnp.bfloat16))
                sides[1][1].append(second.astype(jnp.bfloat16))
            total = None
            for parity in range(2):
                left = jnp.concatenate(
                    [jnp.concatenate(part, axis=1) for part in sides[parity]], axis=0
                )
                for block in range(lane_blocks):
                    copy_of(chunk, parity, block).wait()
                right = jnp.concatenate(
                    [
                        flat[pl.ds((parity * lane_blocks + block) * width + 2 * depth * chunk, 2 * depth)]
                        for block in range(lane_blocks)
                    ],
                    axis=1,
                )
                product = jnp.dot(left, right, preferred_element_type=jnp.float32)
                total = product if total is None else total + product
            if chunk == 0:
                sums[...] = total
            elif chunk < chunks - 1:
                sums[...] += total
            else:
                total = sums[...] + total
                gate_ref[...] = total[:rows].astype(jnp.bfloat16)
                value_ref[...] = total[rows:].astype(jnp.bfloat16)

    whole = pl.BlockSpec(memory_space=pltpu.VMEM)
    return pl.pallas_call(
        body,
        out_shape=[jax.ShapeDtypeStruct((rows, inner_dev), jnp.bfloat16)] * 2,
        in_specs=[whole, pl.BlockSpec(memory_space=pl.ANY)],
        out_specs=[whole] * 2,
        scratch_shapes=[
            pltpu.VMEM((2, lane_blocks, half, 2, 128), jnp.bfloat16),
            pltpu.VMEM((2 * rows, inner_dev), jnp.float32),
            pltpu.SemaphoreType.DMA((chunks, 2, lane_blocks)),
        ],
        name="in_project",
    )(normed, viewed)


def recur(
    gate, value, value_cache, value_kernel, value_offset, step_raw, step_bias, decay_rate,
    skip_gain, out_gain, input_map, output_map, kept_count, scan_state,
):
    rows, inner_dev = gate.shape
    requests = rows // 8
    heads = step_raw.shape[1]
    head_dim = inner_dev // heads
    each = 4

    def body(
        gate_ref, value_ref, cache_ref, ker_ref, off_ref, raw_ref, bias_ref, rate_ref, skip_ref,
        gain_ref, in_ref, out_ref, kept_ref, state_ref,
        gated_ref, square_ref, weighted_ref, decay_ref,
        x_buf, step_buf, after_buf, skip_buf,
    ):
        turn = pl.program_id(0)

        @pl.when(turn == 0)
        def _():
            fresh = value_ref[...].astype(jnp.float32).reshape(requests, 8, inner_dev)
            x_buf[...] = shifted_conv(fresh, cache_ref, ker_ref, off_ref)
            raw = raw_ref[...] + bias_ref[...]
            step = jnp.maximum(raw, 0.0) + jnp.log1p(jnp.exp(-jnp.abs(raw)))
            after = (-step * rate_ref[...]).reshape(requests, 8, heads)
            place = lax.broadcasted_iota(jnp.int32, after.shape, 1)
            for back in (1, 2, 4):
                after = after + jnp.where(place >= back, pltpu.roll(after, back, axis=1), 0.0)
            spread = (
                lax.broadcasted_iota(jnp.int32, (heads, inner_dev), 1) // head_dim
                == lax.broadcasted_iota(jnp.int32, (heads, inner_dev), 0)
            ).astype(jnp.float32)

            def widened(narrow):
                return jnp.dot(
                    narrow, spread, precision=lax.Precision.HIGHEST,
                    preferred_element_type=jnp.float32,
                )

            step_buf[...] = widened(step).reshape(requests, 8, inner_dev)
            after_buf[...] = widened(after.reshape(rows, heads)).reshape(requests, 8, inner_dev)
            skip_buf[...] = widened(jnp.broadcast_to(skip_ref[...], (8, heads)))
            kept_after = jnp.sum(jnp.where(place == kept_ref[...] - 1, after, 0.0), axis=1)
            decay_ref[...] = jnp.exp(kept_after)

        position = lax.broadcasted_iota(jnp.int32, (8, inner_dev), 0)
        skip = skip_buf[0:1]
        for index in range(each):
            request = turn * each + index
            span = pl.ds(request * 8, 8)
            after = after_buf[request]
            x = x_buf[request]
            pushed = step_buf[request] * x
            reads = out_ref[request]
            writes = in_ref[request]
            state = state_ref[index]
            across = (((1,), (1,)), ((), ()))
            carried = lax.dot_general(reads, state, across, preferred_element_type=jnp.float32)
            aligned = lax.dot_general(reads, writes, across, preferred_element_type=jnp.float32)
            total = carried * jnp.exp(after) + skip * x
            for source in range(8):
                gap = jnp.where(position >= source, after - after[source : source + 1], -1e30)
                total = total + jnp.exp(gap) * (
                    aligned[:, source : source + 1] * pushed[source : source + 1]
                )
            gated = total * silu(gate_ref[span].astype(jnp.float32))
            square_ref[span] = jnp.sum(gated * gated, axis=1, keepdims=True)
            gated_ref[span] = (gated * gain_ref[...]).astype(jnp.bfloat16)
            kept = kept_ref[request]
            end = jnp.sum(jnp.where(position == kept - 1, after, 0.0), axis=0, keepdims=True)
            gap = jnp.where(position < kept, end - after, -1e30)
            weighted_ref[request] = (jnp.exp(gap) * pushed).astype(jnp.bfloat16)

    whole = pl.BlockSpec(memory_space=pltpu.VMEM)
    return pl.pallas_call(
        body,
        grid=(requests // each,),
        out_shape=[
            jax.ShapeDtypeStruct((rows, inner_dev), jnp.bfloat16),
            jax.ShapeDtypeStruct((rows, 1), jnp.float32),
            jax.ShapeDtypeStruct((requests, 8, inner_dev), jnp.bfloat16),
            jax.ShapeDtypeStruct((requests, heads), jnp.float32),
        ],
        in_specs=[whole] * 13
        + [pl.BlockSpec((each, inner_dev, 128), lambda turn: (turn, 0, 0))],
        out_specs=[whole] * 4,
        scratch_shapes=[
            pltpu.VMEM((requests, 8, inner_dev), jnp.float32),
            pltpu.VMEM((requests, 8, inner_dev), jnp.float32),
            pltpu.VMEM((requests, 8, inner_dev), jnp.float32),
            pltpu.VMEM((8, inner_dev), jnp.float32),
        ],
        name="recur",
    )(
        gate, value, value_cache, value_kernel, value_offset, step_raw, step_bias, decay_rate,
        skip_gain, out_gain, input_map, output_map, kept_count, scan_state,
    )


def assembled(table, pieces):
    rows = pieces[0].shape[1]

    def body(table_ref, first, second, third, fourth, out_ref):
        for outer, piece in enumerate((first, second, third, fourth)):
            for inner in range(4):
                start = pl.multiple_of(table_ref[4 * outer + inner] * COLS, COLS)
                out_ref[:, pl.ds(start, COLS)] = piece[inner]

    return pl.pallas_call(
        body,
        out_shape=jax.ShapeDtypeStruct((rows, 16 * COLS), jnp.bfloat16),
        in_specs=[pl.BlockSpec(memory_space=pltpu.SMEM)]
        + [pl.BlockSpec(memory_space=pltpu.VMEM)] * 4,
        out_specs=pl.BlockSpec(memory_space=pltpu.VMEM),
        name="assemble_rows",
    )(table, *pieces)


def added(own, received):
    wide = [piece.astype(jnp.float32) for piece in (own, *received)]
    return ((wide[0] + wide[1]) + (wide[2] + wide[3])).astype(jnp.bfloat16)


def stage(pieces, first, second):
    masks = list(zip(first, second))
    received = [None] * 4
    for step in (3, 2, 1):
        received[step] = exchanged(pieces[step], masks[step])
    return received[1:]


def keep_window(sequence, kept_count, width_rows):
    return jax.vmap(
        lambda single, start_row: lax.dynamic_slice_in_dim(single, start_row, width_rows, 0)
    )(sequence, kept_count)


def local(
    tokens,
    norm_gain,
    in_weight,
    group_weight,
    step_weight,
    value_kernel,
    value_offset,
    group_kernel,
    group_offset,
    step_bias,
    decay_rate,
    skip_gain,
    out_gain,
    out_weight,
    scan_state,
    value_cache,
    group_cache,
    accepted,
    draft_lengths,
    live_flags,
):
    requests, positions, model_width = tokens.shape
    row_total = requests * positions
    inner_dev = value_offset.shape[0]
    tap_count = value_kernel.shape[0]
    kept_count = accepted * live_flags
    parity = lax.axis_index("tensor") % 2
    table = chunk_table()
    normed, group_proj, own_conv, step_raw = enter(
        tokens.reshape(row_total, model_width),
        norm_gain[None],
        group_weight,
        step_weight.T,
        group_cache.transpose(1, 0, 2),
        group_kernel,
        group_offset[None],
    )
    other_conv = swapped(own_conv, ("tensor",), 1)
    gate_part, value_part = in_project(normed, in_weight)
    input_map = jnp.where(parity == 0, own_conv, other_conv)
    output_map = jnp.where(parity == 0, other_conv, own_conv)
    scaled, own_squares, weighted, kept_decay = recur(
        gate_part,
        value_part,
        value_cache.transpose(1, 0, 2),
        value_kernel,
        value_offset[None],
        step_raw,
        step_bias[None],
        decay_rate[None],
        skip_gain[None],
        out_gain[None],
        input_map,
        output_map,
        kept_count[:, None, None],
        scan_state.reshape(requests, inner_dev, scan_state.shape[3]),
    )
    other_squares = swapped(own_squares, ("tensor",), 1)
    scale_rows = lax.rsqrt((own_squares + other_squares) / (2 * inner_dev) + EPSILON)
    valid_rows = (jnp.arange(positions)[None, :] < draft_lengths[:, None]) & (
        live_flags[:, None] == 1
    )
    scale = jnp.where(valid_rows.reshape(row_total, 1), scale_rows, 0.0)
    parts = list(out_project(table, scaled, scale, out_weight))
    count = jnp.sum(kept_count).reshape(1)
    count, parts[0] = lax.optimization_barrier((count, parts[0]))
    count = count + swapped(count, DP, 1)
    reduced = added(parts[0], stage(parts, NEAR, FAR))
    count, reduced = lax.optimization_barrier((count, reduced))
    count = count + swapped(count, DP, 2)
    finished = added(reduced, stage([reduced] * 4, FAR, NEAR))
    count, finished = lax.optimization_barrier((count, finished))
    accepted_total = count + swapped(count, DP, 6)
    layer_rows = assembled(table, [finished, *stage([finished] * 4, NEAR, FAR)])
    kept_state = (
        kept_decay[:, :, None, None] * scan_state.astype(jnp.float32)
        + jnp.einsum(
            "rjq,rjn->rqn", weighted, input_map, preferred_element_type=jnp.float32
        ).reshape(scan_state.shape)
    ).astype(jnp.bfloat16)
    value_seq = jnp.concatenate(
        [value_cache, value_part.reshape(requests, positions, inner_dev)], axis=1
    )
    group_seq = jnp.concatenate(
        [group_cache, group_proj.reshape(requests, positions, -1)], axis=1
    )
    value_kept = keep_window(value_seq, kept_count, tap_count - 1)
    group_kept = keep_window(group_seq, kept_count, tap_count - 1)
    return (
        layer_rows.reshape(requests, positions, model_width),
        kept_state,
        value_kept,
        group_kept,
        accepted_total,
    )


def solution(mesh):
    torus = Mesh(mesh.devices.reshape(4, 2, mesh.shape["tensor"]), ("dp_0", "dp_1", "tensor"))
    in_specs = (
        P(DP, None, None),
        P(),
        P(None, None, "tensor"),
        P(None, "tensor"),
        P(None, "tensor"),
        P(None, "tensor"),
        P("tensor"),
        P(None, "tensor"),
        P("tensor"),
        P("tensor"),
        P("tensor"),
        P("tensor"),
        P("tensor"),
        P("tensor", None),
        P(DP, "tensor", None, None),
        P(DP, None, "tensor"),
        P(DP, None, "tensor"),
        P(DP),
        P(DP),
        P(DP),
    )
    out_specs = (
        P(DP, None, None),
        P(DP, "tensor", None, None),
        P(DP, None, "tensor"),
        P(DP, None, "tensor"),
        P(),
    )
    return jax.shard_map(local, mesh=torus, in_specs=in_specs, out_specs=out_specs, check_vma=False)
```

```python
import math

import jax
import jax.numpy as jnp
from jax import lax
from jax.experimental import pallas as pl
from jax.experimental.pallas import tpu as pltpu
from jax.sharding import Mesh
from jax.sharding import PartitionSpec as P

DP = ("dp_0", "dp_1")


EPSILON = 1e-05


ALL = ("dp_0", "dp_1", "tensor")
NEAR = (0, 1, 4, 5)
FAR = (0, 3, 12, 15)
COLS = 256
AHEAD = 2


def swapped(value, axis, mask):
    pairs = [(source, source ^ mask) for source in range(math.prod(lax.axis_size(a) for a in axis))]
    return lax.ppermute(value, axis, pairs)


def exchanged(value, masks):
    tensor = lax.axis_size("tensor")
    total = tensor * lax.axis_size("dp_0") * lax.axis_size("dp_1")
    pairs = [(s, s ^ masks[(s // tensor) % 2]) for s in range(total)]
    return lax.ppermute(value, ALL, pairs)


def chunk_at(outer, inner):
    me = lax.axis_index("tensor")
    core = lax.axis_index("dp_1")
    near = (me ^ (me >> 1)) & 5
    even = near ^ (NEAR[outer] ^ FAR[inner])
    odd = me ^ near ^ (FAR[outer] ^ NEAR[inner])
    return jnp.where(core == 0, even, odd)


def group_scale(own_squares, other_squares, channels):
    return lax.rsqrt((own_squares + other_squares) / channels + EPSILON)


def out_project(gated, out_weight, outers, squares=()):
    rows, inner_dev = gated.shape
    given = len(squares)
    count = len(outers)
    width = 4 * COLS

    def body(gated_ref, weight_ref, *rest):
        parts, (buffer, sems) = rest[given : given + count], rest[given + count :]

        def copies_of(turn):
            copies = []
            for inner in range(4):
                start = pl.multiple_of(chunk_at(outers[turn], inner) * COLS, COLS)
                copies.append(
                    pltpu.make_async_copy(
                        weight_ref.at[:, pl.ds(start, COLS)],
                        buffer.at[turn, :, pl.ds(inner * COLS, COLS)],
                        sems.at[turn, inner],
                    )
                )
            return copies

        copies = [copies_of(turn) for turn in range(count)]
        for turn in range(count):
            for copy in copies[turn]:
                copy.start()
        for turn in range(count):
            for copy in copies[turn]:
                copy.wait()
            part = jnp.dot(gated_ref[...], buffer[turn], preferred_element_type=jnp.float32)
            if given:
                part = part * group_scale(rest[0][...], rest[1][...], 2 * inner_dev)
            part = part.astype(jnp.bfloat16)
            for inner in range(4):
                parts[turn][inner] = part[:, inner * COLS : (inner + 1) * COLS]

    whole = pl.BlockSpec(memory_space=pltpu.VMEM)
    return pl.pallas_call(
        body,
        out_shape=[jax.ShapeDtypeStruct((4, rows, COLS), jnp.bfloat16)] * count,
        in_specs=[whole, pl.BlockSpec(memory_space=pl.ANY)] + [whole] * given,
        out_specs=[whole] * count,
        scratch_shapes=[
            pltpu.VMEM((count, inner_dev, width), jnp.bfloat16),
            pltpu.SemaphoreType.DMA((count, 4)),
        ],
        name="out_project",
    )(gated, out_weight, *squares)


def placed(pieces, outers, earlier=None):
    rows = pieces[0].shape[1]
    count = len(pieces)

    def body(*refs):
        sources, (out_ref, sems) = refs[:count], refs[-2:]
        copies = []
        for index, outer in enumerate(outers):
            for inner in range(4):
                start = pl.multiple_of(chunk_at(outer, inner) * COLS, COLS)
                copies.append(
                    pltpu.make_async_copy(
                        sources[index].at[inner],
                        out_ref.at[:, pl.ds(start, COLS)],
                        sems.at[index, inner],
                    )
                )
        for copy in copies:
            copy.start()
        for copy in copies:
            copy.wait()

    operands = list(pieces) + ([] if earlier is None else [earlier])
    return pl.pallas_call(
        body,
        out_shape=jax.ShapeDtypeStruct((rows, 16 * COLS), jnp.bfloat16),
        in_specs=[pl.BlockSpec(memory_space=pltpu.VMEM)] * count
        + [pl.BlockSpec(memory_space=pl.ANY)] * (len(operands) - count),
        out_specs=pl.BlockSpec(memory_space=pl.ANY),
        scratch_shapes=[pltpu.SemaphoreType.DMA((count, 4))],
        input_output_aliases={} if earlier is None else {count: 0},
        name="place_rows",
    )(*operands)


def added(own, received):
    wide = [piece.astype(jnp.float32) for piece in (own, *received)]
    return ((wide[0] + wide[1]) + (wide[2] + wide[3])).astype(jnp.bfloat16)


def stage(pieces, first, second, steps=(3, 2, 1)):
    masks = list(zip(first, second))
    return {step: exchanged(pieces[step], masks[step]) for step in steps}


def silu(value):
    return value / (1.0 + jnp.exp(-value))


def shifted_conv(fresh, cache_ref, kernel_ref, offset_ref):
    position = lax.broadcasted_iota(jnp.int32, fresh.shape, 1)
    kernel = kernel_ref[...].astype(jnp.float32)
    cache = [cache_ref[i].astype(jnp.float32)[:, None, :] for i in range(3)]
    summed = fresh * kernel[3:4][None] + offset_ref[...].astype(jnp.float32).reshape(1, 1, -1)
    for back in (1, 2, 3):
        moved = pltpu.roll(fresh, back, axis=1)
        for place in range(back):
            moved = jnp.where(position == place, cache[3 - back + place], moved)
        summed = summed + moved * kernel[3 - back : 4 - back][None]
    return silu(summed)


def enter(tokens, norm_gain, group_weight, step_weight, group_cache, group_kernel, group_offset):
    rows, width = tokens.shape
    cols = group_weight.shape[1]
    heads = step_weight.shape[0]

    def body(
        tok_ref, gain_ref, gw_ref, sw_ref, cache_ref, ker_ref, off_ref,
        normed_ref, proj_ref, conv_ref, step_ref,
    ):
        wide = tok_ref[...].astype(jnp.float32)
        scale = lax.rsqrt(jnp.mean(wide * wide, axis=1, keepdims=True) + EPSILON)
        normed = (wide * scale * gain_ref[...]).astype(jnp.bfloat16)
        normed_ref[...] = normed
        proj = jnp.dot(normed, gw_ref[...], preferred_element_type=jnp.float32)
        proj = proj.astype(jnp.bfloat16)
        proj_ref[...] = proj
        step_ref[...] = lax.dot_general(
            normed, sw_ref[...], (((1,), (1,)), ((), ())), preferred_element_type=jnp.float32
        )
        fresh = proj.astype(jnp.float32).reshape(rows // 8, 8, cols)
        conv_ref[...] = shifted_conv(fresh, cache_ref, ker_ref, off_ref).astype(jnp.bfloat16)

    whole = pl.BlockSpec(memory_space=pltpu.VMEM)
    return pl.pallas_call(
        body,
        out_shape=[
            jax.ShapeDtypeStruct((rows, width), jnp.bfloat16),
            jax.ShapeDtypeStruct((rows, cols), jnp.bfloat16),
            jax.ShapeDtypeStruct((rows // 8, 8, cols), jnp.bfloat16),
            jax.ShapeDtypeStruct((rows, heads), jnp.float32),
        ],
        in_specs=[whole] * 7,
        out_specs=[whole] * 4,
        name="enter",
    )(tokens, norm_gain, group_weight, step_weight, group_cache, group_kernel, group_offset)


def in_project(normed, in_weight):
    rows, width = normed.shape
    half = width // 2
    lane_blocks = in_weight.shape[2] // 128
    inner_dev = in_weight.shape[2]
    pairs = lane_blocks // 2
    halves = 2
    depth = half // halves
    viewed = in_weight.reshape(half, 2, 2, lane_blocks, 128).transpose(0, 1, 3, 2, 4)

    def body(normed_ref, weight_ref, gate_ref, value_ref, buffer, left, sems):
        def copies_of(turn):
            pair, part = turn
            span = pl.ds(part * depth, depth)
            return [
                pltpu.make_async_copy(
                    weight_ref.at[span, parity, block],
                    buffer.at[parity, block, span],
                    sems.at[part, parity, block],
                )
                for parity in range(2)
                for block in (2 * pair, 2 * pair + 1)
            ]

        turns = [(pair, part) for pair in range(pairs) for part in range(halves)]
        for turn in turns[:AHEAD]:
            for copy in copies_of(turn):
                copy.start()
        flat = buffer.reshape(2 * lane_blocks * width, 128)
        even = lax.broadcasted_iota(jnp.int32, (rows, 128), 1) % 2 == 0
        for lane in range(0, width, 128):
            span = slice(lane, lane + 128)
            piece = normed_ref[:, span].astype(jnp.float32)
            first = jnp.where(even, piece, 0.0)
            second = jnp.where(even, 0.0, piece)
            left[0, 0:rows, span] = first.astype(jnp.bfloat16)
            left[0, rows:, span] = pltpu.roll(first, 1, axis=1).astype(jnp.bfloat16)
            left[1, 0:rows, span] = pltpu.roll(second, 127, axis=1).astype(jnp.bfloat16)
            left[1, rows:, span] = second.astype(jnp.bfloat16)
        total = None
        for index, (pair, part) in enumerate(turns):
            for copy in copies_of((pair, part)):
                copy.wait()
            if index + AHEAD < len(turns):
                for copy in copies_of(turns[index + AHEAD]):
                    copy.start()
            for parity in range(2):
                right = jnp.concatenate(
                    [
                        flat[pl.ds((parity * lane_blocks + block) * width + 2 * depth * part, 2 * depth)]
                        for block in (2 * pair, 2 * pair + 1)
                    ],
                    axis=1,
                )
                product = jnp.dot(
                    left[parity, :, 2 * depth * part : 2 * depth * (part + 1)],
                    right,
                    preferred_element_type=jnp.float32,
                )
                total = product if total is None else total + product
            if part == halves - 1:
                span = slice(256 * pair, 256 * pair + 256)
                gate_ref[:, span] = total[:rows].astype(jnp.bfloat16)
                value_ref[:, span] = total[rows:].astype(jnp.bfloat16)
                total = None

    whole = pl.BlockSpec(memory_space=pltpu.VMEM)
    return pl.pallas_call(
        body,
        out_shape=[jax.ShapeDtypeStruct((rows, inner_dev), jnp.bfloat16)] * 2,
        in_specs=[whole, pl.BlockSpec(memory_space=pl.ANY)],
        out_specs=[whole] * 2,
        scratch_shapes=[
            pltpu.VMEM((2, lane_blocks, half, 2, 128), jnp.bfloat16),
            pltpu.VMEM((2, 2 * rows, width), jnp.bfloat16),
            pltpu.SemaphoreType.DMA((halves, 2, lane_blocks)),
        ],
        name="in_project",
    )(normed, viewed)


def recur(
    gate, value, value_cache, value_kernel, value_offset, step_raw, step_bias, decay_rate,
    skip_gain, out_gain, own_map, other_map, accepted, draft_lengths, live_flags, scan_state,
):
    rows, inner_dev = gate.shape
    requests = rows // 8
    heads = step_raw.shape[1]
    head_dim = inner_dev // heads
    each = 12

    def body(
        gate_ref, value_ref, cache_ref, ker_ref, off_ref, raw_ref, bias_ref, rate_ref, skip_ref,
        gain_ref, own_ref, other_ref, accepted_ref, length_ref, live_ref, state_ref,
        gated_ref, square_ref, weighted_ref, decay_ref,
        x_buf, step_buf, after_buf, skip_buf, narrow_buf,
    ):
        turn = pl.program_id(0)
        first_half = lax.axis_index("tensor") % 2 == 0

        @pl.when(turn == 0)
        def _():
            fresh = value_ref[...].astype(jnp.float32).reshape(requests, 8, inner_dev)
            x_buf[...] = shifted_conv(fresh, cache_ref, ker_ref, off_ref)
            raw = raw_ref[...] + bias_ref[...]
            step = jnp.maximum(raw, 0.0) + jnp.log1p(jnp.exp(-jnp.abs(raw)))
            after = (-step * rate_ref[...]).reshape(requests, 8, heads)
            place = lax.broadcasted_iota(jnp.int32, after.shape, 1)
            for back in (1, 2, 4):
                after = after + jnp.where(place >= back, pltpu.roll(after, back, axis=1), 0.0)
            spread = (
                lax.broadcasted_iota(jnp.int32, (heads, inner_dev), 1) // head_dim
                == lax.broadcasted_iota(jnp.int32, (heads, inner_dev), 0)
            ).astype(jnp.float32)

            def widened(narrow):
                return jnp.dot(
                    narrow, spread, precision=lax.Precision.HIGHEST,
                    preferred_element_type=jnp.float32,
                )

            step_buf[...] = widened(step).reshape(requests, 8, inner_dev)
            after_buf[...] = widened(after.reshape(rows, heads)).reshape(requests, 8, inner_dev)
            skip_buf[...] = widened(jnp.broadcast_to(skip_ref[...], (8, heads)))
            narrow_buf[...] = after

        position = lax.broadcasted_iota(jnp.int32, (8, inner_dev), 0)
        skip = skip_buf[0:1]
        for index in range(each):
            request = turn * each + index
            span = pl.ds(request * 8, 8)
            after = after_buf[request]
            x = x_buf[request]
            pushed = step_buf[request] * x
            own, other = own_ref[request], other_ref[request]
            reads = jnp.where(first_half, other, own)
            writes = jnp.where(first_half, own, other)
            state = state_ref[index]
            across = (((1,), (1,)), ((), ()))
            carried = lax.dot_general(reads, state, across, preferred_element_type=jnp.float32)
            aligned = lax.dot_general(reads, writes, across, preferred_element_type=jnp.float32)
            total = carried * jnp.exp(after) + skip * x
            for source in range(8):
                gap = jnp.where(position >= source, after - after[source : source + 1], -1e30)
                total = total + jnp.exp(gap) * (
                    aligned[:, source : source + 1] * pushed[source : source + 1]
                )
            gated = total * silu(gate_ref[span].astype(jnp.float32))
            square_ref[span] = jnp.sum(gated * gated, axis=1, keepdims=True)
            length = jnp.where(live_ref[request] == 1, length_ref[request], 0)
            gated = jnp.where(position < length, gated * gain_ref[...], 0.0)
            gated_ref[span] = gated.astype(jnp.bfloat16)
            kept = accepted_ref[request] * live_ref[request]
            narrow = narrow_buf[request]
            place = lax.broadcasted_iota(jnp.int32, narrow.shape, 0)
            narrow = jnp.sum(jnp.where(place == kept - 1, narrow, 0.0), axis=0, keepdims=True)
            decay_ref[pl.ds(request, 1)] = jnp.exp(narrow)
            end = jnp.sum(jnp.where(position == kept - 1, after, 0.0), axis=0, keepdims=True)
            gap = jnp.where(position < kept, end - after, -1e30)
            weighted_ref[request] = (jnp.exp(gap) * pushed).astype(jnp.bfloat16)

    whole = pl.BlockSpec(memory_space=pltpu.VMEM)
    return pl.pallas_call(
        body,
        grid=(requests // each,),
        out_shape=[
            jax.ShapeDtypeStruct((rows, inner_dev), jnp.bfloat16),
            jax.ShapeDtypeStruct((rows, 1), jnp.float32),
            jax.ShapeDtypeStruct((requests, 8, inner_dev), jnp.bfloat16),
            jax.ShapeDtypeStruct((requests, heads), jnp.float32),
        ],
        in_specs=[whole] * 12
        + [pl.BlockSpec(memory_space=pltpu.SMEM)] * 3
        + [pl.BlockSpec((each, inner_dev, 128), lambda turn: (turn, 0, 0))],
        out_specs=[whole] * 4,
        scratch_shapes=[
            pltpu.VMEM((requests, 8, inner_dev), jnp.float32),
            pltpu.VMEM((requests, 8, inner_dev), jnp.float32),
            pltpu.VMEM((requests, 8, inner_dev), jnp.float32),
            pltpu.VMEM((8, inner_dev), jnp.float32),
            pltpu.VMEM((requests, 8, heads), jnp.float32),
        ],
        name="recur",
    )(
        gate, value, value_cache, value_kernel, value_offset, step_raw, step_bias, decay_rate,
        skip_gain, out_gain, own_map, other_map, accepted, draft_lengths, live_flags, scan_state,
    )


def keep_window(sequence, kept_count, width_rows):
    return jax.vmap(
        lambda single, start_row: lax.dynamic_slice_in_dim(single, start_row, width_rows, 0)
    )(sequence, kept_count)


def local(
    tokens,
    norm_gain,
    in_weight,
    group_weight,
    step_weight,
    value_kernel,
    value_offset,
    group_kernel,
    group_offset,
    step_bias,
    decay_rate,
    skip_gain,
    out_gain,
    out_weight,
    scan_state,
    value_cache,
    group_cache,
    accepted,
    draft_lengths,
    live_flags,
):
    requests, positions, model_width = tokens.shape
    row_total = requests * positions
    inner_dev = value_offset.shape[0]
    tap_count = value_kernel.shape[0]
    kept_count = accepted * live_flags
    parity = lax.axis_index("tensor") % 2
    normed, group_proj, own_conv, step_raw = enter(
        tokens.reshape(row_total, model_width),
        norm_gain[None],
        group_weight,
        step_weight.T,
        group_cache.transpose(1, 0, 2),
        group_kernel,
        group_offset[None],
    )
    other_conv = swapped(own_conv, ("tensor",), 1)
    gate_part, value_part = in_project(normed, in_weight)
    input_map = jnp.where(parity == 0, own_conv, other_conv)
    scaled, own_squares, weighted, kept_decay = recur(
        gate_part,
        value_part,
        value_cache.transpose(1, 0, 2),
        value_kernel,
        value_offset,
        step_raw,
        step_bias[None],
        decay_rate[None],
        skip_gain[None],
        out_gain[None],
        own_conv,
        other_conv,
        accepted,
        draft_lengths,
        live_flags,
        scan_state.reshape(requests, inner_dev, scan_state.shape[3]),
    )
    other_squares = swapped(own_squares, ("tensor",), 1)
    (raw,) = out_project(scaled, out_weight, (3,))
    squares = (own_squares, other_squares)
    scale = group_scale(*squares, 2 * inner_dev)
    farthest = (raw.astype(jnp.float32) * scale).astype(jnp.bfloat16)
    received = stage({3: farthest}, NEAR, FAR, (3,))
    scaled, farthest = lax.optimization_barrier((scaled, farthest))
    second, first, own = out_project(scaled, out_weight, (2, 1, 0), squares)
    own, value_part, group_proj = lax.optimization_barrier((own, value_part, group_proj))
    received.update(stage({2: second, 1: first}, NEAR, FAR, (2, 1)))
    count = jnp.sum(kept_count).reshape(1)
    count, own = lax.optimization_barrier((count, own))
    count = count + swapped(count, DP, 1)
    reduced = added(own, [received[step] for step in (1, 2, 3)])
    count, reduced = lax.optimization_barrier((count, reduced))
    count = count + swapped(count, DP, 2)
    received = stage([reduced] * 4, FAR, NEAR)
    accepted_total = count + swapped(count, DP, 6)
    accepted_total, received[1] = lax.optimization_barrier((accepted_total, received[1]))
    finished = added(reduced, [received[step] for step in (1, 2, 3)])
    finished, weighted = lax.optimization_barrier((finished, weighted))
    received = stage([finished] * 4, NEAR, FAR)
    layer_rows = placed([finished, received[3]], (0, 3))
    layer_rows = placed([received[2], received[1]], (2, 1), layer_rows)
    kept_state = (
        kept_decay[:, :, None, None] * scan_state.astype(jnp.float32)
        + jnp.einsum(
            "rjq,rjn->rqn", weighted, input_map, preferred_element_type=jnp.float32
        ).reshape(scan_state.shape)
    ).astype(jnp.bfloat16)
    value_seq = jnp.concatenate(
        [value_cache, value_part.reshape(requests, positions, inner_dev)], axis=1
    )
    group_seq = jnp.concatenate(
        [group_cache, group_proj.reshape(requests, positions, -1)], axis=1
    )
    value_kept = keep_window(value_seq, kept_count, tap_count - 1)
    group_kept = keep_window(group_seq, kept_count, tap_count - 1)
    return (
        layer_rows.reshape(requests, positions, model_width),
        kept_state,
        value_kept,
        group_kept,
        accepted_total,
    )


def solution(mesh):
    torus = Mesh(mesh.devices.reshape(4, 2, mesh.shape["tensor"]), ("dp_0", "dp_1", "tensor"))
    in_specs = (
        P(DP, None, None),
        P(),
        P(None, None, "tensor"),
        P(None, "tensor"),
        P(None, "tensor"),
        P(None, "tensor"),
        P("tensor"),
        P(None, "tensor"),
        P("tensor"),
        P("tensor"),
        P("tensor"),
        P("tensor"),
        P("tensor"),
        P("tensor", None),
        P(DP, "tensor", None, None),
        P(DP, None, "tensor"),
        P(DP, None, "tensor"),
        P(DP),
        P(DP),
        P(DP),
    )
    out_specs = (
        P(DP, None, None),
        P(DP, "tensor", None, None),
        P(DP, None, "tensor"),
        P(DP, None, "tensor"),
        P(),
    )
    return jax.shard_map(local, mesh=torus, in_specs=in_specs, out_specs=out_specs, check_vma=False)
```

```python
import math

import jax
import jax.numpy as jnp
from jax import lax
from jax.experimental import pallas as pl
from jax.experimental.pallas import tpu as pltpu
from jax.sharding import Mesh
from jax.sharding import PartitionSpec as P

DP = ("dp_0", "dp_1")


EPSILON = 1e-05


ALL = ("dp_0", "dp_1", "tensor")
NEAR = (0, 1, 4, 5)
FAR = (0, 3, 12, 15)
COLS = 256
AHEAD = 2


def swapped(value, axis, mask):
    pairs = [(source, source ^ mask) for source in range(math.prod(lax.axis_size(a) for a in axis))]
    return lax.ppermute(value, axis, pairs)


def exchanged(value, masks):
    tensor = lax.axis_size("tensor")
    total = tensor * lax.axis_size("dp_0") * lax.axis_size("dp_1")
    pairs = [(s, s ^ masks[(s // tensor) % 2]) for s in range(total)]
    return lax.ppermute(value, ALL, pairs)


def chunk_at(outer, inner):
    me = lax.axis_index("tensor")
    core = lax.axis_index("dp_1")
    near = (me ^ (me >> 1)) & 5
    even = near ^ (NEAR[outer] ^ FAR[inner])
    odd = me ^ near ^ (FAR[outer] ^ NEAR[inner])
    return jnp.where(core == 0, even, odd)


def group_scale(own_squares, other_squares, channels):
    return lax.rsqrt((own_squares + other_squares) / channels + EPSILON)


def out_project(gated, out_weight, outers, squares=()):
    rows, inner_dev = gated.shape
    given = len(squares)
    count = len(outers)
    width = 4 * COLS

    def body(gated_ref, weight_ref, *rest):
        parts, (buffer, sems) = rest[given : given + count], rest[given + count :]

        def copies_of(turn):
            copies = []
            for inner in range(4):
                start = pl.multiple_of(chunk_at(outers[turn], inner) * COLS, COLS)
                copies.append(
                    pltpu.make_async_copy(
                        weight_ref.at[:, pl.ds(start, COLS)],
                        buffer.at[turn, :, pl.ds(inner * COLS, COLS)],
                        sems.at[turn, inner],
                    )
                )
            return copies

        copies = [copies_of(turn) for turn in range(count)]
        for turn in range(count):
            for copy in copies[turn]:
                copy.start()
        for turn in range(count):
            for copy in copies[turn]:
                copy.wait()
            part = jnp.dot(gated_ref[...], buffer[turn], preferred_element_type=jnp.float32)
            if given:
                part = part * group_scale(rest[0][...], rest[1][...], 2 * inner_dev)
            part = part.astype(jnp.bfloat16)
            for inner in range(4):
                parts[turn][inner] = part[:, inner * COLS : (inner + 1) * COLS]

    whole = pl.BlockSpec(memory_space=pltpu.VMEM)
    return pl.pallas_call(
        body,
        out_shape=[jax.ShapeDtypeStruct((4, rows, COLS), jnp.bfloat16)] * count,
        in_specs=[whole, pl.BlockSpec(memory_space=pl.ANY)] + [whole] * given,
        out_specs=[whole] * count,
        scratch_shapes=[
            pltpu.VMEM((count, inner_dev, width), jnp.bfloat16),
            pltpu.SemaphoreType.DMA((count, 4)),
        ],
        name="out_project",
    )(gated, out_weight, *squares)


def placed(pieces, outers, earlier=None):
    rows = pieces[0].shape[1]
    count = len(pieces)

    def body(*refs):
        sources, (out_ref, sems) = refs[:count], refs[-2:]
        copies = []
        for index, outer in enumerate(outers):
            for inner in range(4):
                start = pl.multiple_of(chunk_at(outer, inner) * COLS, COLS)
                copies.append(
                    pltpu.make_async_copy(
                        sources[index].at[inner],
                        out_ref.at[:, pl.ds(start, COLS)],
                        sems.at[index, inner],
                    )
                )
        for copy in copies:
            copy.start()
        for copy in copies:
            copy.wait()

    operands = list(pieces) + ([] if earlier is None else [earlier])
    return pl.pallas_call(
        body,
        out_shape=jax.ShapeDtypeStruct((rows, 16 * COLS), jnp.bfloat16),
        in_specs=[pl.BlockSpec(memory_space=pltpu.VMEM)] * count
        + [pl.BlockSpec(memory_space=pl.ANY)] * (len(operands) - count),
        out_specs=pl.BlockSpec(memory_space=pl.ANY),
        scratch_shapes=[pltpu.SemaphoreType.DMA((count, 4))],
        input_output_aliases={} if earlier is None else {count: 0},
        name="place_rows",
    )(*operands)


def added(own, received):
    wide = [piece.astype(jnp.float32) for piece in (own, *received)]
    return ((wide[0] + wide[1]) + (wide[2] + wide[3])).astype(jnp.bfloat16)


def stage(pieces, first, second, steps=(3, 2, 1)):
    masks = list(zip(first, second))
    return {step: exchanged(pieces[step], masks[step]) for step in steps}


def silu(value):
    return value / (1.0 + jnp.exp(-value))


def shifted_conv(fresh, cache_ref, kernel_ref, offset_ref):
    position = lax.broadcasted_iota(jnp.int32, fresh.shape, 1)
    kernel = kernel_ref[...].astype(jnp.float32)
    cache = [cache_ref[i].astype(jnp.float32)[:, None, :] for i in range(3)]
    summed = fresh * kernel[3:4][None] + offset_ref[...].astype(jnp.float32).reshape(1, 1, -1)
    for back in (1, 2, 3):
        moved = pltpu.roll(fresh, back, axis=1)
        for place in range(back):
            moved = jnp.where(position == place, cache[3 - back + place], moved)
        summed = summed + moved * kernel[3 - back : 4 - back][None]
    return silu(summed)


def enter(tokens, norm_gain, group_weight, step_weight, group_cache, group_kernel, group_offset):
    rows, width = tokens.shape
    cols = group_weight.shape[1]
    heads = step_weight.shape[0]

    def body(
        tok_ref, gain_ref, gw_ref, sw_ref, cache_ref, ker_ref, off_ref,
        normed_ref, proj_ref, conv_ref, step_ref,
    ):
        wide = tok_ref[...].astype(jnp.float32)
        scale = lax.rsqrt(jnp.mean(wide * wide, axis=1, keepdims=True) + EPSILON)
        normed = (wide * scale * gain_ref[...]).astype(jnp.bfloat16)
        normed_ref[...] = normed
        proj = jnp.dot(normed, gw_ref[...], preferred_element_type=jnp.float32)
        proj = proj.astype(jnp.bfloat16)
        proj_ref[...] = proj
        step_ref[...] = lax.dot_general(
            normed, sw_ref[...], (((1,), (1,)), ((), ())), preferred_element_type=jnp.float32
        )
        fresh = proj.astype(jnp.float32).reshape(rows // 8, 8, cols)
        conv_ref[...] = shifted_conv(fresh, cache_ref, ker_ref, off_ref).astype(jnp.bfloat16)

    whole = pl.BlockSpec(memory_space=pltpu.VMEM)
    return pl.pallas_call(
        body,
        out_shape=[
            jax.ShapeDtypeStruct((rows, width), jnp.bfloat16),
            jax.ShapeDtypeStruct((rows, cols), jnp.bfloat16),
            jax.ShapeDtypeStruct((rows // 8, 8, cols), jnp.bfloat16),
            jax.ShapeDtypeStruct((rows, heads), jnp.float32),
        ],
        in_specs=[whole] * 7,
        out_specs=[whole] * 4,
        name="enter",
    )(tokens, norm_gain, group_weight, step_weight, group_cache, group_kernel, group_offset)


def in_project(normed, in_weight):
    rows, width = normed.shape
    half = width // 2
    lane_blocks = in_weight.shape[2] // 128
    inner_dev = in_weight.shape[2]
    pairs = lane_blocks // 2
    halves = 2
    depth = half // halves
    viewed = in_weight.reshape(half, 2, 2, lane_blocks, 128).transpose(0, 1, 3, 2, 4)

    def body(source_ref, weight_ref, gate_ref, value_ref, normed_ref, buffer, left, sems, sem):
        def copies_of(turn):
            pair, part = turn
            span = pl.ds(part * depth, depth)
            return [
                pltpu.make_async_copy(
                    weight_ref.at[span, parity, block],
                    buffer.at[parity, block, span],
                    sems.at[part, parity, block],
                )
                for parity in range(2)
                for block in (2 * pair, 2 * pair + 1)
            ]

        turns = [(pair, part) for pair in range(pairs) for part in range(halves)]
        for turn in turns[:AHEAD]:
            for copy in copies_of(turn):
                copy.start()
        entering = pltpu.make_async_copy(source_ref, normed_ref, sem)
        entering.start()
        entering.wait()
        flat = buffer.reshape(2 * lane_blocks * width, 128)
        even = lax.broadcasted_iota(jnp.int32, (rows, 128), 1) % 2 == 0
        for lane in range(0, width, 128):
            span = slice(lane, lane + 128)
            piece = normed_ref[:, span].astype(jnp.float32)
            first = jnp.where(even, piece, 0.0)
            second = jnp.where(even, 0.0, piece)
            left[0, 0:rows, span] = first.astype(jnp.bfloat16)
            left[0, rows:, span] = pltpu.roll(first, 1, axis=1).astype(jnp.bfloat16)
            left[1, 0:rows, span] = pltpu.roll(second, 127, axis=1).astype(jnp.bfloat16)
            left[1, rows:, span] = second.astype(jnp.bfloat16)
        total = None
        for index, (pair, part) in enumerate(turns):
            for copy in copies_of((pair, part)):
                copy.wait()
            if index + AHEAD < len(turns):
                for copy in copies_of(turns[index + AHEAD]):
                    copy.start()
            for parity in range(2):
                right = jnp.concatenate(
                    [
                        flat[pl.ds((parity * lane_blocks + block) * width + 2 * depth * part, 2 * depth)]
                        for block in (2 * pair, 2 * pair + 1)
                    ],
                    axis=1,
                )
                product = jnp.dot(
                    left[parity, :, 2 * depth * part : 2 * depth * (part + 1)],
                    right,
                    preferred_element_type=jnp.float32,
                )
                total = product if total is None else total + product
            if part == halves - 1:
                span = slice(256 * pair, 256 * pair + 256)
                gate_ref[:, span] = total[:rows].astype(jnp.bfloat16)
                value_ref[:, span] = total[rows:].astype(jnp.bfloat16)
                total = None

    whole = pl.BlockSpec(memory_space=pltpu.VMEM)
    return pl.pallas_call(
        body,
        out_shape=[jax.ShapeDtypeStruct((rows, inner_dev), jnp.bfloat16)] * 2,
        in_specs=[pl.BlockSpec(memory_space=pl.ANY)] * 2,
        out_specs=[whole] * 2,
        scratch_shapes=[
            pltpu.VMEM((rows, width), jnp.bfloat16),
            pltpu.VMEM((2, lane_blocks, half, 2, 128), jnp.bfloat16),
            pltpu.VMEM((2, 2 * rows, width), jnp.bfloat16),
            pltpu.SemaphoreType.DMA((halves, 2, lane_blocks)),
            pltpu.SemaphoreType.DMA,
        ],
        name="in_project",
    )(normed, viewed)


def recur(
    gate, value, value_cache, value_kernel, value_offset, step_raw, step_bias, decay_rate,
    skip_gain, out_gain, own_map, other_map, accepted, draft_lengths, live_flags, scan_state,
):
    rows, inner_dev = gate.shape
    requests = rows // 8
    heads = step_raw.shape[1]
    head_dim = inner_dev // heads
    each = 12

    def body(
        gate_ref, value_ref, cache_ref, ker_ref, off_ref, raw_ref, bias_ref, rate_ref, skip_ref,
        gain_ref, own_ref, other_ref, accepted_ref, length_ref, live_ref, state_ref,
        gated_ref, square_ref, weighted_ref, decay_ref,
        x_buf, step_buf, after_buf, skip_buf, narrow_buf,
    ):
        turn = pl.program_id(0)
        first_half = lax.axis_index("tensor") % 2 == 0

        @pl.when(turn == 0)
        def _():
            fresh = value_ref[...].astype(jnp.float32).reshape(requests, 8, inner_dev)
            x_buf[...] = shifted_conv(fresh, cache_ref, ker_ref, off_ref)
            raw = raw_ref[...] + bias_ref[...]
            step = jnp.maximum(raw, 0.0) + jnp.log1p(jnp.exp(-jnp.abs(raw)))
            after = (-step * rate_ref[...]).reshape(requests, 8, heads)
            place = lax.broadcasted_iota(jnp.int32, after.shape, 1)
            for back in (1, 2, 4):
                after = after + jnp.where(place >= back, pltpu.roll(after, back, axis=1), 0.0)
            spread = (
                lax.broadcasted_iota(jnp.int32, (heads, inner_dev), 1) // head_dim
                == lax.broadcasted_iota(jnp.int32, (heads, inner_dev), 0)
            ).astype(jnp.float32)

            def widened(narrow):
                return jnp.dot(
                    narrow, spread, precision=lax.Precision.HIGHEST,
                    preferred_element_type=jnp.float32,
                )

            step_buf[...] = widened(step).reshape(requests, 8, inner_dev)
            after_buf[...] = widened(after.reshape(rows, heads)).reshape(requests, 8, inner_dev)
            skip_buf[...] = widened(jnp.broadcast_to(skip_ref[...], (8, heads)))
            narrow_buf[...] = after

        position = lax.broadcasted_iota(jnp.int32, (8, inner_dev), 0)
        skip = skip_buf[0:1]
        for index in range(each):
            request = turn * each + index
            span = pl.ds(request * 8, 8)
            after = after_buf[request]
            x = x_buf[request]
            pushed = step_buf[request] * x
            own, other = own_ref[request], other_ref[request]
            reads = jnp.where(first_half, other, own)
            writes = jnp.where(first_half, own, other)
            state = state_ref[index]
            across = (((1,), (1,)), ((), ()))
            carried = lax.dot_general(reads, state, across, preferred_element_type=jnp.float32)
            aligned = lax.dot_general(reads, writes, across, preferred_element_type=jnp.float32)
            total = carried * jnp.exp(after) + skip * x
            for source in range(8):
                gap = jnp.where(position >= source, after - after[source : source + 1], -1e30)
                total = total + jnp.exp(gap) * (
                    aligned[:, source : source + 1] * pushed[source : source + 1]
                )
            gated = total * silu(gate_ref[span].astype(jnp.float32))
            square_ref[span] = jnp.sum(gated * gated, axis=1, keepdims=True)
            length = jnp.where(live_ref[request] == 1, length_ref[request], 0)
            gated = jnp.where(position < length, gated * gain_ref[...], 0.0)
            gated_ref[span] = gated.astype(jnp.bfloat16)
            kept = accepted_ref[request] * live_ref[request]
            narrow = narrow_buf[request]
            place = lax.broadcasted_iota(jnp.int32, narrow.shape, 0)
            narrow = jnp.sum(jnp.where(place == kept - 1, narrow, 0.0), axis=0, keepdims=True)
            decay_ref[pl.ds(request, 1)] = jnp.exp(narrow)
            end = jnp.sum(jnp.where(position == kept - 1, after, 0.0), axis=0, keepdims=True)
            gap = jnp.where(position < kept, end - after, -1e30)
            weighted_ref[request] = (jnp.exp(gap) * pushed).astype(jnp.bfloat16)

    whole = pl.BlockSpec(memory_space=pltpu.VMEM)
    return pl.pallas_call(
        body,
        grid=(requests // each,),
        out_shape=[
            jax.ShapeDtypeStruct((rows, inner_dev), jnp.bfloat16),
            jax.ShapeDtypeStruct((rows, 1), jnp.float32),
            jax.ShapeDtypeStruct((requests, 8, inner_dev), jnp.bfloat16),
            jax.ShapeDtypeStruct((requests, heads), jnp.float32),
        ],
        in_specs=[whole] * 12
        + [pl.BlockSpec(memory_space=pltpu.SMEM)] * 3
        + [pl.BlockSpec((each, inner_dev, 128), lambda turn: (turn, 0, 0))],
        out_specs=[whole] * 4,
        scratch_shapes=[
            pltpu.VMEM((requests, 8, inner_dev), jnp.float32),
            pltpu.VMEM((requests, 8, inner_dev), jnp.float32),
            pltpu.VMEM((requests, 8, inner_dev), jnp.float32),
            pltpu.VMEM((8, inner_dev), jnp.float32),
            pltpu.VMEM((requests, 8, heads), jnp.float32),
        ],
        name="recur",
    )(
        gate, value, value_cache, value_kernel, value_offset, step_raw, step_bias, decay_rate,
        skip_gain, out_gain, own_map, other_map, accepted, draft_lengths, live_flags, scan_state,
    )


def keep_window(sequence, kept_count, width_rows):
    return jax.vmap(
        lambda single, start_row: lax.dynamic_slice_in_dim(single, start_row, width_rows, 0)
    )(sequence, kept_count)


def local(
    tokens,
    norm_gain,
    in_weight,
    group_weight,
    step_weight,
    value_kernel,
    value_offset,
    group_kernel,
    group_offset,
    step_bias,
    decay_rate,
    skip_gain,
    out_gain,
    out_weight,
    scan_state,
    value_cache,
    group_cache,
    accepted,
    draft_lengths,
    live_flags,
):
    requests, positions, model_width = tokens.shape
    row_total = requests * positions
    inner_dev = value_offset.shape[0]
    tap_count = value_kernel.shape[0]
    kept_count = accepted * live_flags
    parity = lax.axis_index("tensor") % 2
    normed, group_proj, own_conv, step_raw = enter(
        tokens.reshape(row_total, model_width),
        norm_gain[None],
        group_weight,
        step_weight.T,
        group_cache.transpose(1, 0, 2),
        group_kernel,
        group_offset[None],
    )
    other_conv = swapped(own_conv, ("tensor",), 1)
    gate_part, value_part = in_project(normed, in_weight)
    input_map = jnp.where(parity == 0, own_conv, other_conv)
    scaled, own_squares, weighted, kept_decay = recur(
        gate_part,
        value_part,
        value_cache.transpose(1, 0, 2),
        value_kernel,
        value_offset,
        step_raw,
        step_bias[None],
        decay_rate[None],
        skip_gain[None],
        out_gain[None],
        own_conv,
        other_conv,
        accepted,
        draft_lengths,
        live_flags,
        scan_state.reshape(requests, inner_dev, scan_state.shape[3]),
    )
    other_squares = swapped(own_squares, ("tensor",), 1)
    (raw,) = out_project(scaled, out_weight, (3,))
    squares = (own_squares, other_squares)
    scale = group_scale(*squares, 2 * inner_dev)
    farthest = (raw.astype(jnp.float32) * scale).astype(jnp.bfloat16)
    received = stage({3: farthest}, NEAR, FAR, (3,))
    scaled, farthest = lax.optimization_barrier((scaled, farthest))
    second, first, own = out_project(scaled, out_weight, (2, 1, 0), squares)
    own, value_part, group_proj = lax.optimization_barrier((own, value_part, group_proj))
    received.update(stage({2: second, 1: first}, NEAR, FAR, (2, 1)))
    kept_count, own = lax.optimization_barrier((kept_count, own))
    count = jnp.sum(kept_count).reshape(1)
    count = count + swapped(count, DP, 1)
    reduced = added(own, [received[step] for step in (1, 2, 3)])
    count, reduced, weighted = lax.optimization_barrier((count, reduced, weighted))
    count = count + swapped(count, DP, 2)
    received = stage([reduced] * 4, FAR, NEAR)
    finished = added(reduced, [received[step] for step in (1, 2, 3)])
    count, finished = lax.optimization_barrier((count, finished))
    accepted_total = count + swapped(count, DP, 6)
    received = stage([finished] * 4, NEAR, FAR)
    layer_rows = placed([finished, received[3]], (0, 3))
    layer_rows = placed([received[2], received[1]], (2, 1), layer_rows)
    kept_state = (
        kept_decay[:, :, None, None] * scan_state.astype(jnp.float32)
        + jnp.einsum(
            "rjq,rjn->rqn", weighted, input_map, preferred_element_type=jnp.float32
        ).reshape(scan_state.shape)
    ).astype(jnp.bfloat16)
    value_seq = jnp.concatenate(
        [value_cache, value_part.reshape(requests, positions, inner_dev)], axis=1
    )
    group_seq = jnp.concatenate(
        [group_cache, group_proj.reshape(requests, positions, -1)], axis=1
    )
    value_kept = keep_window(value_seq, kept_count, tap_count - 1)
    group_kept = keep_window(group_seq, kept_count, tap_count - 1)
    return (
        layer_rows.reshape(requests, positions, model_width),
        kept_state,
        value_kept,
        group_kept,
        accepted_total,
    )


def solution(mesh):
    torus = Mesh(mesh.devices.reshape(4, 2, mesh.shape["tensor"]), ("dp_0", "dp_1", "tensor"))
    in_specs = (
        P(DP, None, None),
        P(),
        P(None, None, "tensor"),
        P(None, "tensor"),
        P(None, "tensor"),
        P(None, "tensor"),
        P("tensor"),
        P(None, "tensor"),
        P("tensor"),
        P("tensor"),
        P("tensor"),
        P("tensor"),
        P("tensor"),
        P("tensor", None),
        P(DP, "tensor", None, None),
        P(DP, None, "tensor"),
        P(DP, None, "tensor"),
        P(DP),
        P(DP),
        P(DP),
    )
    out_specs = (
        P(DP, None, None),
        P(DP, "tensor", None, None),
        P(DP, None, "tensor"),
        P(DP, None, "tensor"),
        P(),
    )
    return jax.shard_map(local, mesh=torus, in_specs=in_specs, out_specs=out_specs, check_vma=False)
```

```python
import math

import jax
import jax.numpy as jnp
from jax import lax
from jax.experimental import pallas as pl
from jax.experimental.pallas import tpu as pltpu
from jax.sharding import Mesh
from jax.sharding import PartitionSpec as P

DP = ("dp_0", "dp_1")


EPSILON = 1e-05


ALL = ("dp_0", "dp_1", "tensor")
NEAR = (0, 1, 4, 5)
FAR = (0, 3, 12, 15)
COLS = 256


def swapped(value, axis, mask):
    pairs = [(source, source ^ mask) for source in range(math.prod(lax.axis_size(a) for a in axis))]
    return lax.ppermute(value, axis, pairs)


def exchanged(value, masks):
    tensor = lax.axis_size("tensor")
    total = tensor * lax.axis_size("dp_0") * lax.axis_size("dp_1")
    pairs = [(s, s ^ masks[(s // tensor) % 2]) for s in range(total)]
    return lax.ppermute(value, ALL, pairs)


def chunk_at(outer, inner):
    me = lax.axis_index("tensor")
    core = lax.axis_index("dp_1")
    near = (me ^ (me >> 1)) & 5
    even = near ^ (NEAR[outer] ^ FAR[inner])
    odd = me ^ near ^ (FAR[outer] ^ NEAR[inner])
    return jnp.where(core == 0, even, odd)


def group_scale(own_squares, other_squares, channels):
    return lax.rsqrt((own_squares + other_squares) / channels + EPSILON)


def out_project(gated, out_weight, outers, squares=()):
    rows, inner_dev = gated.shape
    given = len(squares)
    count = len(outers)
    width = 4 * COLS

    def body(gated_ref, weight_ref, *rest):
        parts, (buffer, sems) = rest[given : given + count], rest[given + count :]

        def copies_of(turn):
            copies = []
            for inner in range(4):
                start = pl.multiple_of(chunk_at(outers[turn], inner) * COLS, COLS)
                copies.append(
                    pltpu.make_async_copy(
                        weight_ref.at[:, pl.ds(start, COLS)],
                        buffer.at[turn, :, pl.ds(inner * COLS, COLS)],
                        sems.at[turn, inner],
                    )
                )
            return copies

        copies = [copies_of(turn) for turn in range(count)]
        for turn in range(count):
            for copy in copies[turn]:
                copy.start()
        for turn in range(count):
            for copy in copies[turn]:
                copy.wait()
            part = jnp.dot(gated_ref[...], buffer[turn], preferred_element_type=jnp.float32)
            if given:
                part = part * group_scale(rest[0][...], rest[1][...], 2 * inner_dev)
            part = part.astype(jnp.bfloat16)
            for inner in range(4):
                parts[turn][inner] = part[:, inner * COLS : (inner + 1) * COLS]

    whole = pl.BlockSpec(memory_space=pltpu.VMEM)
    return pl.pallas_call(
        body,
        out_shape=[jax.ShapeDtypeStruct((4, rows, COLS), jnp.bfloat16)] * count,
        in_specs=[whole, pl.BlockSpec(memory_space=pl.ANY)] + [whole] * given,
        out_specs=[whole] * count,
        scratch_shapes=[
            pltpu.VMEM((count, inner_dev, width), jnp.bfloat16),
            pltpu.SemaphoreType.DMA((count, 4)),
        ],
        name="out_project",
    )(gated, out_weight, *squares)


def placed(pieces, outers, earlier=None):
    rows = pieces[0].shape[1]
    count = len(pieces)

    def body(*refs):
        sources, (out_ref, sems) = refs[:count], refs[-2:]
        copies = []
        for index, outer in enumerate(outers):
            for inner in range(4):
                start = pl.multiple_of(chunk_at(outer, inner) * COLS, COLS)
                copies.append(
                    pltpu.make_async_copy(
                        sources[index].at[inner],
                        out_ref.at[:, pl.ds(start, COLS)],
                        sems.at[index, inner],
                    )
                )
        for copy in copies:
            copy.start()
        for copy in copies:
            copy.wait()

    operands = list(pieces) + ([] if earlier is None else [earlier])
    return pl.pallas_call(
        body,
        out_shape=jax.ShapeDtypeStruct((rows, 16 * COLS), jnp.bfloat16),
        in_specs=[pl.BlockSpec(memory_space=pltpu.VMEM)] * count
        + [pl.BlockSpec(memory_space=pl.ANY)] * (len(operands) - count),
        out_specs=pl.BlockSpec(memory_space=pl.ANY),
        scratch_shapes=[pltpu.SemaphoreType.DMA((count, 4))],
        input_output_aliases={} if earlier is None else {count: 0},
        name="place_rows",
    )(*operands)


def added(own, received):
    wide = [piece.astype(jnp.float32) for piece in (own, *received)]
    return ((wide[0] + wide[1]) + (wide[2] + wide[3])).astype(jnp.bfloat16)


def stage(pieces, first, second, steps=(3, 2, 1)):
    masks = list(zip(first, second))
    return {step: exchanged(pieces[step], masks[step]) for step in steps}


def silu(value):
    return value / (1.0 + jnp.exp(-value))


def shifted_conv(fresh, cache_ref, kernel_ref, offset_ref):
    position = lax.broadcasted_iota(jnp.int32, fresh.shape, 1)
    kernel = kernel_ref[...].astype(jnp.float32)
    cache = [cache_ref[i].astype(jnp.float32)[:, None, :] for i in range(3)]
    summed = fresh * kernel[3:4][None] + offset_ref[...].astype(jnp.float32).reshape(1, 1, -1)
    for back in (1, 2, 3):
        moved = pltpu.roll(fresh, back, axis=1)
        for place in range(back):
            moved = jnp.where(position == place, cache[3 - back + place], moved)
        summed = summed + moved * kernel[3 - back : 4 - back][None]
    return silu(summed)


def enter(tokens, norm_gain, group_weight, step_weight, group_cache, group_kernel, group_offset):
    rows, width = tokens.shape
    cols = group_weight.shape[1]
    heads = step_weight.shape[0]

    def body(
        tok_ref, gain_ref, gw_ref, sw_ref, cache_ref, ker_ref, off_ref,
        normed_ref, proj_ref, conv_ref, step_ref,
    ):
        wide = tok_ref[...].astype(jnp.float32)
        scale = lax.rsqrt(jnp.mean(wide * wide, axis=1, keepdims=True) + EPSILON)
        normed = (wide * scale * gain_ref[...]).astype(jnp.bfloat16)
        normed_ref[...] = normed
        proj = jnp.dot(normed, gw_ref[...], preferred_element_type=jnp.float32)
        proj = proj.astype(jnp.bfloat16)
        proj_ref[...] = proj
        step_ref[...] = lax.dot_general(
            normed, sw_ref[...], (((1,), (1,)), ((), ())), preferred_element_type=jnp.float32
        )
        fresh = proj.astype(jnp.float32).reshape(rows // 8, 8, cols)
        conv_ref[...] = shifted_conv(fresh, cache_ref, ker_ref, off_ref).astype(jnp.bfloat16)

    whole = pl.BlockSpec(memory_space=pltpu.VMEM)
    return pl.pallas_call(
        body,
        out_shape=[
            jax.ShapeDtypeStruct((rows, width), jnp.bfloat16),
            jax.ShapeDtypeStruct((rows, cols), jnp.bfloat16),
            jax.ShapeDtypeStruct((rows // 8, 8, cols), jnp.bfloat16),
            jax.ShapeDtypeStruct((rows, heads), jnp.float32),
        ],
        in_specs=[whole] * 7,
        out_specs=[whole] * 4,
        name="enter",
    )(tokens, norm_gain, group_weight, step_weight, group_cache, group_kernel, group_offset)


def in_project(normed, in_weight):
    rows, width = normed.shape
    half = width // 2
    lane_blocks = in_weight.shape[2] // 128
    inner_dev = in_weight.shape[2]
    turns = 4
    depth = half // turns
    viewed = in_weight.reshape(half, 2, 2, lane_blocks, 128).transpose(0, 1, 3, 2, 4)

    def body(normed_ref, weight_ref, gate_ref, value_ref, buffer, left, sums, sems):
        def copies_of(turn):
            span = pl.ds(turn * depth, depth)
            return [
                pltpu.make_async_copy(
                    weight_ref.at[span, parity, block],
                    buffer.at[parity, block, span],
                    sems.at[turn, parity, block],
                )
                for parity in range(2)
                for block in range(lane_blocks)
            ]

        for turn in range(turns):
            for copy in copies_of(turn):
                copy.start()
        flat = buffer.reshape(2 * lane_blocks * width, 128)
        even = lax.broadcasted_iota(jnp.int32, (rows, 128), 1) % 2 == 0
        for lane in range(0, width, 128):
            span = slice(lane, lane + 128)
            piece = normed_ref[:, span].astype(jnp.float32)
            first = jnp.where(even, piece, 0.0)
            second = jnp.where(even, 0.0, piece)
            left[0, 0:rows, span] = first.astype(jnp.bfloat16)
            left[0, rows:, span] = pltpu.roll(first, 1, axis=1).astype(jnp.bfloat16)
            left[1, 0:rows, span] = pltpu.roll(second, 127, axis=1).astype(jnp.bfloat16)
            left[1, rows:, span] = second.astype(jnp.bfloat16)
        for turn in range(turns):
            for copy in copies_of(turn):
                copy.wait()
            begin = 2 * depth * turn
            total = None
            for parity in range(2):
                right = jnp.concatenate(
                    [
                        flat[pl.ds((parity * lane_blocks + block) * width + begin, 2 * depth)]
                        for block in range(lane_blocks)
                    ],
                    axis=1,
                )
                product = jnp.dot(
                    left[parity, :, begin : begin + 2 * depth],
                    right,
                    preferred_element_type=jnp.float32,
                )
                total = product if total is None else total + product
            if turn == 0:
                sums[...] = total
            elif turn < turns - 1:
                sums[...] += total
            else:
                total = sums[...] + total
                gate_ref[...] = total[:rows].astype(jnp.bfloat16)
                value_ref[...] = total[rows:].astype(jnp.bfloat16)

    whole = pl.BlockSpec(memory_space=pltpu.VMEM)
    return pl.pallas_call(
        body,
        out_shape=[jax.ShapeDtypeStruct((rows, inner_dev), jnp.bfloat16)] * 2,
        in_specs=[whole, pl.BlockSpec(memory_space=pl.ANY)],
        out_specs=[whole] * 2,
        scratch_shapes=[
            pltpu.VMEM((2, lane_blocks, half, 2, 128), jnp.bfloat16),
            pltpu.VMEM((2, 2 * rows, width), jnp.bfloat16),
            pltpu.VMEM((2 * rows, inner_dev), jnp.float32),
            pltpu.SemaphoreType.DMA((turns, 2, lane_blocks)),
        ],
        name="in_project",
    )(normed, viewed)


def recur(
    gate, value, value_cache, value_kernel, value_offset, step_raw, step_bias, decay_rate,
    skip_gain, out_gain, own_map, other_map, accepted, draft_lengths, live_flags, scan_state,
):
    rows, inner_dev = gate.shape
    requests = rows // 8
    heads = step_raw.shape[1]
    head_dim = inner_dev // heads
    each = 12

    def body(
        gate_ref, value_ref, cache_ref, ker_ref, off_ref, raw_ref, bias_ref, rate_ref, skip_ref,
        gain_ref, own_ref, other_ref, accepted_ref, length_ref, live_ref, state_ref,
        gated_ref, square_ref, weighted_ref, decay_ref,
        x_buf, step_buf, after_buf, skip_buf, narrow_buf,
    ):
        turn = pl.program_id(0)
        first_half = lax.axis_index("tensor") % 2 == 0

        @pl.when(turn == 0)
        def _():
            fresh = value_ref[...].astype(jnp.float32).reshape(requests, 8, inner_dev)
            x_buf[...] = shifted_conv(fresh, cache_ref, ker_ref, off_ref)
            raw = raw_ref[...] + bias_ref[...]
            step = jnp.maximum(raw, 0.0) + jnp.log1p(jnp.exp(-jnp.abs(raw)))
            after = (-step * rate_ref[...]).reshape(requests, 8, heads)
            place = lax.broadcasted_iota(jnp.int32, after.shape, 1)
            for back in (1, 2, 4):
                after = after + jnp.where(place >= back, pltpu.roll(after, back, axis=1), 0.0)
            spread = (
                lax.broadcasted_iota(jnp.int32, (heads, inner_dev), 1) // head_dim
                == lax.broadcasted_iota(jnp.int32, (heads, inner_dev), 0)
            ).astype(jnp.float32)

            def widened(narrow):
                return jnp.dot(
                    narrow, spread, precision=lax.Precision.HIGHEST,
                    preferred_element_type=jnp.float32,
                )

            step_buf[...] = widened(step).reshape(requests, 8, inner_dev)
            after_buf[...] = widened(after.reshape(rows, heads)).reshape(requests, 8, inner_dev)
            skip_buf[...] = widened(jnp.broadcast_to(skip_ref[...], (8, heads)))
            narrow_buf[...] = after

        position = lax.broadcasted_iota(jnp.int32, (8, inner_dev), 0)
        skip = skip_buf[0:1]
        for index in range(each):
            request = turn * each + index
            span = pl.ds(request * 8, 8)
            after = after_buf[request]
            x = x_buf[request]
            pushed = step_buf[request] * x
            own, other = own_ref[request], other_ref[request]
            reads = jnp.where(first_half, other, own)
            writes = jnp.where(first_half, own, other)
            state = state_ref[index]
            across = (((1,), (1,)), ((), ()))
            carried = lax.dot_general(reads, state, across, preferred_element_type=jnp.float32)
            aligned = lax.dot_general(reads, writes, across, preferred_element_type=jnp.float32)
            total = carried * jnp.exp(after) + skip * x
            for source in range(8):
                gap = jnp.where(position >= source, after - after[source : source + 1], -1e30)
                total = total + jnp.exp(gap) * (
                    aligned[:, source : source + 1] * pushed[source : source + 1]
                )
            gated = total * silu(gate_ref[span].astype(jnp.float32))
            square_ref[span] = jnp.sum(gated * gated, axis=1, keepdims=True)
            length = jnp.where(live_ref[request] == 1, length_ref[request], 0)
            gated = jnp.where(position < length, gated * gain_ref[...], 0.0)
            gated_ref[span] = gated.astype(jnp.bfloat16)
            kept = accepted_ref[request] * live_ref[request]
            narrow = narrow_buf[request]
            place = lax.broadcasted_iota(jnp.int32, narrow.shape, 0)
            narrow = jnp.sum(jnp.where(place == kept - 1, narrow, 0.0), axis=0, keepdims=True)
            decay_ref[pl.ds(request, 1)] = jnp.exp(narrow)
            end = jnp.sum(jnp.where(position == kept - 1, after, 0.0), axis=0, keepdims=True)
            gap = jnp.where(position < kept, end - after, -1e30)
            weighted_ref[request] = (jnp.exp(gap) * pushed).astype(jnp.bfloat16)

    whole = pl.BlockSpec(memory_space=pltpu.VMEM)
    return pl.pallas_call(
        body,
        grid=(requests // each,),
        out_shape=[
            jax.ShapeDtypeStruct((rows, inner_dev), jnp.bfloat16),
            jax.ShapeDtypeStruct((rows, 1), jnp.float32),
            jax.ShapeDtypeStruct((requests, 8, inner_dev), jnp.bfloat16),
            jax.ShapeDtypeStruct((requests, heads), jnp.float32),
        ],
        in_specs=[whole] * 12
        + [pl.BlockSpec(memory_space=pltpu.SMEM)] * 3
        + [pl.BlockSpec((each, inner_dev, 128), lambda turn: (turn, 0, 0))],
        out_specs=[whole] * 4,
        scratch_shapes=[
            pltpu.VMEM((requests, 8, inner_dev), jnp.float32),
            pltpu.VMEM((requests, 8, inner_dev), jnp.float32),
            pltpu.VMEM((requests, 8, inner_dev), jnp.float32),
            pltpu.VMEM((8, inner_dev), jnp.float32),
            pltpu.VMEM((requests, 8, heads), jnp.float32),
        ],
        name="recur",
    )(
        gate, value, value_cache, value_kernel, value_offset, step_raw, step_bias, decay_rate,
        skip_gain, out_gain, own_map, other_map, accepted, draft_lengths, live_flags, scan_state,
    )


def keep_window(sequence, kept_count, width_rows):
    return jax.vmap(
        lambda single, start_row: lax.dynamic_slice_in_dim(single, start_row, width_rows, 0)
    )(sequence, kept_count)


def local(
    tokens,
    norm_gain,
    in_weight,
    group_weight,
    step_weight,
    value_kernel,
    value_offset,
    group_kernel,
    group_offset,
    step_bias,
    decay_rate,
    skip_gain,
    out_gain,
    out_weight,
    scan_state,
    value_cache,
    group_cache,
    accepted,
    draft_lengths,
    live_flags,
):
    requests, positions, model_width = tokens.shape
    row_total = requests * positions
    inner_dev = value_offset.shape[0]
    tap_count = value_kernel.shape[0]
    kept_count = accepted * live_flags
    parity = lax.axis_index("tensor") % 2
    normed, group_proj, own_conv, step_raw = enter(
        tokens.reshape(row_total, model_width),
        norm_gain[None],
        group_weight,
        step_weight.T,
        group_cache.transpose(1, 0, 2),
        group_kernel,
        group_offset[None],
    )
    other_conv = swapped(own_conv, ("tensor",), 1)
    gate_part, value_part = in_project(normed, in_weight)
    input_map = jnp.where(parity == 0, own_conv, other_conv)
    scaled, own_squares, weighted, kept_decay = recur(
        gate_part,
        value_part,
        value_cache.transpose(1, 0, 2),
        value_kernel,
        value_offset,
        step_raw,
        step_bias[None],
        decay_rate[None],
        skip_gain[None],
        out_gain[None],
        own_conv,
        other_conv,
        accepted,
        draft_lengths,
        live_flags,
        scan_state.reshape(requests, inner_dev, scan_state.shape[3]),
    )
    other_squares = swapped(own_squares, ("tensor",), 1)
    (raw,) = out_project(scaled, out_weight, (3,))
    squares = (own_squares, other_squares)
    scale = group_scale(*squares, 2 * inner_dev)
    farthest = (raw.astype(jnp.float32) * scale).astype(jnp.bfloat16)
    received = stage({3: farthest}, NEAR, FAR, (3,))
    scaled, farthest = lax.optimization_barrier((scaled, farthest))
    second, first, own = out_project(scaled, out_weight, (2, 1, 0), squares)
    own, value_part, group_proj = lax.optimization_barrier((own, value_part, group_proj))
    received.update(stage({2: second, 1: first}, NEAR, FAR, (2, 1)))
    kept_count, own = lax.optimization_barrier((kept_count, own))
    count = jnp.sum(kept_count).reshape(1)
    count = count + swapped(count, DP, 1)
    reduced = added(own, [received[step] for step in (1, 2, 3)])
    count, reduced, weighted = lax.optimization_barrier((count, reduced, weighted))
    count = count + swapped(count, DP, 2)
    received = stage([reduced] * 4, FAR, NEAR)
    finished = added(reduced, [received[step] for step in (1, 2, 3)])
    count, finished = lax.optimization_barrier((count, finished))
    accepted_total = count + swapped(count, DP, 6)
    received = stage([finished] * 4, NEAR, FAR)
    layer_rows = placed([finished, received[3]], (0, 3))
    layer_rows = placed([received[2], received[1]], (2, 1), layer_rows)
    kept_state = (
        kept_decay[:, :, None, None] * scan_state.astype(jnp.float32)
        + jnp.einsum(
            "rjq,rjn->rqn", weighted, input_map, preferred_element_type=jnp.float32
        ).reshape(scan_state.shape)
    ).astype(jnp.bfloat16)
    value_seq = jnp.concatenate(
        [value_cache, value_part.reshape(requests, positions, inner_dev)], axis=1
    )
    group_seq = jnp.concatenate(
        [group_cache, group_proj.reshape(requests, positions, -1)], axis=1
    )
    value_kept = keep_window(value_seq, kept_count, tap_count - 1)
    group_kept = keep_window(group_seq, kept_count, tap_count - 1)
    return (
        layer_rows.reshape(requests, positions, model_width),
        kept_state,
        value_kept,
        group_kept,
        accepted_total,
    )


def solution(mesh):
    torus = Mesh(mesh.devices.reshape(4, 2, mesh.shape["tensor"]), ("dp_0", "dp_1", "tensor"))
    in_specs = (
        P(DP, None, None),
        P(),
        P(None, None, "tensor"),
        P(None, "tensor"),
        P(None, "tensor"),
        P(None, "tensor"),
        P("tensor"),
        P(None, "tensor"),
        P("tensor"),
        P("tensor"),
        P("tensor"),
        P("tensor"),
        P("tensor"),
        P("tensor", None),
        P(DP, "tensor", None, None),
        P(DP, None, "tensor"),
        P(DP, None, "tensor"),
        P(DP),
        P(DP),
        P(DP),
    )
    out_specs = (
        P(DP, None, None),
        P(DP, "tensor", None, None),
        P(DP, None, "tensor"),
        P(DP, None, "tensor"),
        P(),
    )
    return jax.shard_map(local, mesh=torus, in_specs=in_specs, out_specs=out_specs, check_vma=False)
```
